128 devices in a mesh: data: 1, time: 128 (over z, y, x, core).
Axes of the slice: x: 4, y: 4, z: 4, core: 2. Of those that a mesh axis runs over, the one named last changes fastest.
Arguments:
- x_init: float32 [4, 64, 768], P('data')
- w_in: bfloat16 [768, 3072], replicated
- w_out: bfloat16 [3072, 768], replicated
- mod_gamma: bfloat16 [1024, 3072], P('time')
- mod_beta: bfloat16 [1024, 3072], P('time')
- step_size: float32 [1024], P('time')
Outputs:
- output: float32 [4, 64, 768], P('data')
All inputs are finite; a program needn't handle non-finite values.
Results may differ from the reference program's by a relative error of at most 0.001.
Values are sent between devices in bfloat16 or wider.
A program may use at most 1 GiB of HBM per device.

```python
import jax
import jax.numpy as jnp
from jax import lax

SAMPLES = 4
TOKENS = 64
CHANNELS = 768
HIDDEN = 3072
NUM_STEPS = 1024
SWEEPS = 4


def setup_inputs(seed: int = 0, part: int = 0) -> dict:
    base_key = jax.random.key(seed)
    part_key = jax.random.fold_in(base_key, part)
    sub_keys = jax.random.split(base_key, 6)
    x_init = jax.random.normal(part_key, (SAMPLES, TOKENS, CHANNELS), jnp.float32)
    w_in = (jax.random.normal(sub_keys[0], (CHANNELS, HIDDEN), jnp.float32) * CHANNELS ** -0.5).astype(jnp.bfloat16)
    w_out = (jax.random.normal(sub_keys[1], (HIDDEN, CHANNELS), jnp.float32) * HIDDEN ** -0.5).astype(jnp.bfloat16)
    mod_gamma = (0.5 * jax.random.normal(sub_keys[2], (NUM_STEPS, HIDDEN), jnp.float32)).astype(jnp.bfloat16)
    mod_beta = jax.random.normal(sub_keys[3], (NUM_STEPS, HIDDEN), jnp.float32).astype(jnp.bfloat16)
    total_time = 1.0 + 2.0 * jax.random.uniform(sub_keys[4], (), jnp.float32)
    step_size = (0.5 + jax.random.uniform(sub_keys[5], (NUM_STEPS,), jnp.float32)) * (total_time / NUM_STEPS)
    return {"x_init": x_init, "w_in": w_in, "w_out": w_out, "mod_gamma": mod_gamma, "mod_beta": mod_beta, "step_size": step_size}


def drift_of(latents, w_in, w_out, gamma_j, beta_j, h_step):
    pre_act = jnp.dot(latents.astype(jnp.bfloat16).reshape(-1, CHANNELS), w_in, preferred_element_type=jnp.float32)
    hidden_act = jax.nn.gelu(pre_act * (1.0 + gamma_j.astype(jnp.float32)) + beta_j.astype(jnp.float32), approximate=True).astype(jnp.bfloat16)
    proj_out = jnp.dot(hidden_act, w_out, preferred_element_type=jnp.float32)
    return h_step * proj_out.reshape(latents.shape)


def reference(x_init, w_in, w_out, mod_gamma, mod_beta, step_size):
    run_init = jnp.zeros((SWEEPS,) + x_init.shape, jnp.float32)

    def step_body(run_sums, step_in):
        gamma_j, beta_j, h_step = step_in
        latents = jnp.concatenate([x_init[None], x_init[None] + run_sums[:-1]], axis=0)
        return run_sums + drift_of(latents, w_in, w_out, gamma_j, beta_j, h_step), None

    run_sums, _ = lax.scan(step_body, run_init, (mod_gamma, mod_beta, step_size))
    return x_init + run_sums[-1]
```

```python
import math

import jax
import jax.numpy as jnp
from jax import lax
from jax.experimental import pallas as pl
from jax.experimental.pallas import tpu as pltpu
from jax.sharding import PartitionSpec as P

C = 768; D = 3072; T = 1024
K0 = math.sqrt(2.0 / math.pi)
K1 = 2.0 * K0
K3 = 8.0 * 0.044715 * K0
f32 = jnp.float32; bf16 = jnp.bfloat16

def gelu_half(w):
    u = w * (K1 + K3 * (w * w))
    return w * jnp.tanh(u) + w

def make(J=64, CH=1024, LAG=2):
    NB = T // J
    NCH = D // CH
    SUB = 256
    PC = C // NCH
    RING = 3 * LAG + 1
    M = 2 * J

    def kernel(x0_ref, win_ref, wout_ref, gam_ref, bet_ref, h_ref, y_ref,
               g_ring, b_ring, xs, fs, a0, rs, s_acc):
        rowid = lax.broadcasted_iota(jnp.int32, (8, PC), 0)
        xpad = jnp.concatenate([x0_ref[...], jnp.zeros((14, C), f32)], 0).astype(bf16)
        a0[...] = jnp.dot(xpad, win_ref[...], preferred_element_type=f32)[0:8]
        for s in range(3):
            for k in range(2):
                rs[s, k] = jnp.broadcast_to(x0_ref[k:k + 1, :], (8, C))
        s_acc[...] = jnp.zeros_like(s_acc)

        def body(t, n, act, pre):
            par = lax.rem(t, 2)
            off = n * CH
            if pre:
                pcol = pl.ds(pl.multiple_of(n * PC, PC), PC)
                for s in pre:
                    blk = t - 1 - LAG * s
                    for k in range(2):
                        carry = rs[s, k, :, pcol]
                        for p in range(J // 8):
                            r0 = k * J + p * 8
                            hv = h_ref[pl.ds(pl.multiple_of(blk * J, J) + p * 8, 8), :]
                            v = fs[1 - par, s, pl.ds(r0, 8), pcol] * jnp.concatenate([hv] * (PC // 128), 1)
                            c = v
                            for sh in (1, 2, 4):
                                c = c + jnp.where(rowid >= sh, pltpu.roll(c, sh, 0), 0.0)
                            fs[1 - par, s, pl.ds(r0, 8), pcol] = carry + (c - v)
                            carry = carry + jnp.broadcast_to(c[7:8, :], (8, PC))
                        rs[s, k, :, pcol] = carry
                        xs[1 - par, pl.ds((s * 2 + k) * J, J), pcol] = fs[1 - par, s, pl.ds(k * J, J), pcol].astype(bf16)
            mm = [s for s in act if s >= 1]
            outs = [s for s in act if s <= 2]
            slot = {s: lax.rem(t - LAG * s, RING) for s in act}
            gparts = []
            facc = None
            for i in range(CH // SUB):
                cols = pl.ds(pl.multiple_of(off + i * SUB, SUB), SUB)
                A = None
                if mm:
                    lo = (mm[0] - 1) * M; hi = mm[-1] * M
                    A = jnp.dot(xs[par, lo:hi, :], win_ref[:, cols], preferred_element_type=f32)
                gs = []
                for s in act:
                    if s == 0:
                        rows = pl.ds(pl.multiple_of(t * J, J), J)
                        g1 = gam_ref[rows, cols].astype(f32) * 0.5 + 0.5
                        b1 = bet_ref[rows, cols].astype(f32) * 0.5
                        g_ring[slot[0], :, cols] = g1
                        b_ring[slot[0], :, cols] = b1
                        for k in range(2):
                            ak = a0[k:k + 1, cols]
                            gs.append(gelu_half(ak * g1 + b1).astype(bf16))
                    else:
                        g1 = g_ring[slot[s], :, cols]
                        b1 = b_ring[slot[s], :, cols]
                        base = (s - mm[0]) * M
                        for k in range(2):
                            ak = A[base + k * J: base + (k + 1) * J]
                            gv = gelu_half(ak * g1 + b1).astype(bf16)
                            if s <= 2:
                                gs.append(gv)
                            else:
                                blk = t - LAG * 3
                                tot = s_acc[k, :, cols]
                                for p in range(J // 8):
                                    hv = h_ref[pl.ds(pl.multiple_of(blk * J, J) + p * 8, 8), :]
                                    tot = tot + gv[p * 8:(p + 1) * 8].astype(f32) * jnp.concatenate([hv] * (SUB // 128), 1)
                                s_acc[k, :, cols] = tot
                if outs:
                    G = jnp.concatenate(gs, 0) if len(gs) > 1 else gs[0]
                    gparts.append(G)
            if outs:
                G = jnp.concatenate(gparts, 1) if len(gparts) > 1 else gparts[0]
                d = jnp.dot(G, wout_ref[pl.ds(pl.multiple_of(off, CH), CH), :], preferred_element_type=f32)
                for q, s in enumerate(outs):
                    part = d[q * M:(q + 1) * M]

                    @pl.when(n == 0)
                    def _(): fs[par, s] = part

                    @pl.when(n != 0)
                    def _(): fs[par, s] += part

        nsteps = NB + 3 * LAG
        def sets(t):
            act = tuple(s for s in range(4) if 0 <= t - LAG * s < NB)
            pre = tuple(s for s in range(3) if 0 <= t - 1 - LAG * s < NB)
            return act, pre
        t = 0
        while t < nsteps:
            e = t
            while e < nsteps and sets(e) == sets(t):
                e += 1
            act, pre = sets(t)
            if e - t == 1:
                lax.fori_loop(0, NCH, lambda n, _, t=t, act=act, pre=pre: (body(jnp.int32(t), n, act, pre), 0)[1], 0)
            else:
                lax.fori_loop(0, NCH * (e - t), lambda i, _, t=t, act=act, pre=pre: (body(t + i // NCH, i % NCH, act, pre), 0)[1], 0)
            t = e

        st = jnp.concatenate([jnp.sum(s_acc[k], axis=0, keepdims=True) for k in range(2)], 0)
        h1 = st.astype(bf16); r1 = st - h1.astype(f32)
        h2 = r1.astype(bf16); r2 = r1 - h2.astype(f32)
        h3 = r2.astype(bf16)
        lhs = jnp.concatenate([h1.astype(f32), h2.astype(f32), h3.astype(f32), jnp.zeros((10, D), f32)], 0).astype(bf16)
        o = jnp.dot(lhs, wout_ref[...], preferred_element_type=f32)
        y_ref[...] = x0_ref[...] + (o[0:2] + (o[2:4] + o[4:6]))

    scratch = [
        pltpu.VMEM((RING, J, D), f32), pltpu.VMEM((RING, J, D), f32),
        pltpu.VMEM((2, 3 * M, C), bf16), pltpu.VMEM((2, 3, M, C), f32),
        pltpu.VMEM((8, D), f32), pltpu.VMEM((3, 2, 8, C), f32), pltpu.VMEM((2, 8, D), f32),
    ]
    return pl.pallas_call(kernel, out_shape=jax.ShapeDtypeStruct((2, C), f32),
        in_specs=[pl.BlockSpec(memory_space=pltpu.VMEM)] * 6,
        out_specs=pl.BlockSpec(memory_space=pltpu.VMEM),
        scratch_shapes=scratch,
        compiler_params=pltpu.CompilerParams(vmem_limit_bytes=62 * 2**20))


def solution(mesh):
    run = make()

    def local_run(x_init, w_in, w_out, mod_gamma, mod_beta, step_size):
        me = lax.axis_index("time")
        x2 = lax.dynamic_slice(x_init.reshape(256, C), (2 * me, 0), (2, C))
        gam = lax.all_gather(mod_gamma, "time", axis=0, tiled=True)
        bet = lax.all_gather(mod_beta, "time", axis=0, tiled=True)
        h = lax.all_gather(step_size, "time", axis=0, tiled=True)
        hb = jnp.broadcast_to(h[:, None], (T, 128))
        y2 = run(x2, w_in, w_out, gam, bet, hb)
        y = lax.all_gather(y2, "time", axis=0, tiled=True)
        return y.reshape(x_init.shape)

    return jax.shard_map(local_run, mesh=mesh, in_specs=(P("data", None, None), P(None, None), P(None, None), P("time", None), P("time", None), P("time")), out_specs=P("data", None, None), check_vma=False)
```

```python
import math

import jax
import jax.numpy as jnp
from jax import lax
from jax.experimental import pallas as pl
from jax.experimental.pallas import tpu as pltpu
from jax.sharding import PartitionSpec as P

C = 768
D = 3072
T = 1024
J = 64
CH = 1024
LAG = 2
D2LAG = 2
SUB = 256
NB = T // J
NCH = D // CH
NS = CH // SUB
PC = C // NCH
RING = 3 * LAG + 1
M = 2 * J
K0 = math.sqrt(2.0 / math.pi)
K1 = 2.0 * K0
K3 = 8.0 * 0.044715 * K0
f32 = jnp.float32
bf16 = jnp.bfloat16


def gelu_half(w):
    return w * jnp.tanh(w * (K1 + K3 * (w * w))) + w


def kernel(x_hbm, win_hbm, wout_hbm, gam_hbm, bet_hbm, h_hbm, y_ref,
           gb, hb, win_ref, wout_ref, x8, g_ring, b_ring, xs0, xs1, fs0, fs1, a0, rs, s_acc, yall,
           local_sem, send_sem, sendh_sem, in_sem, inh_sem, x_sem, xh_sem, d_sem, dh_sem, ysend_sem, y_sem):
    me = lax.axis_index("time")
    c = lax.rem(me, 2)
    x = lax.rem(me // 2, 4)
    y = lax.rem(me // 8, 4)
    z = me // 32

    def peer(zz, yy, xx, cc):
        return {"time": ((zz * 4 + yy) * 4 + xx) * 2 + cc}

    def chip(zz, yy, xx):
        return (zz * 4 + yy) * 4 + xx

    mychip = chip(z, y, x)
    zpeers = [peer(lax.rem(z + d, 4), y, x, c) for d in (1, 3, 2)]
    ypeers = [peer(z, lax.rem(y + d, 4), x, c) for d in (1, 3, 2)]
    xpeers = [peer(z, y, lax.rem(x + d, 4), c) for d in (1, 3, 2)]
    partner = peer(z, y, x, 1 - c)

    own = [pltpu.make_async_copy(gam_hbm, gb.at[mychip, c, 0], local_sem.at[0]),
           pltpu.make_async_copy(bet_hbm, gb.at[mychip, c, 1], local_sem.at[1]),
           pltpu.make_async_copy(h_hbm, hb.at[mychip, c], local_sem.at[2])]
    weights = [pltpu.make_async_copy(x_hbm.at[pl.ds(pl.multiple_of((me // 4) * 8, 8), 8)], x8, local_sem.at[3]),
               pltpu.make_async_copy(win_hbm, win_ref, local_sem.at[4]),
               pltpu.make_async_copy(wout_hbm, wout_ref, local_sem.at[5])]
    for cp in own + weights:
        cp.start()

    barrier = pltpu.get_barrier_semaphore()
    for p in zpeers + ypeers + xpeers + [partner]:
        pl.semaphore_signal(barrier, inc=1, device_id=p, device_id_type=pl.DeviceIdType.MESH)
    pl.semaphore_wait(barrier, 10)
    for cp in own:
        cp.wait()

    def send(src, dst, ssem, rsem, dev):
        pltpu.make_async_remote_copy(src_ref=src, dst_ref=dst, send_sem=ssem, recv_sem=rsem,
                                     device_id=dev, device_id_type=pl.DeviceIdType.MESH).start()

    def send_chunk(q, cc, peers, gsem, hsem):
        for p in peers:
            send(gb.at[q, cc], gb.at[q, cc], send_sem, gsem, p)
            send(hb.at[q, cc], hb.at[q, cc], sendh_sem, hsem, p)

    def wait_chunks(n, gsem, hsem):
        g = gb.at[pl.ds(0, n), 0]
        h = hb.at[pl.ds(0, n), 0]
        pltpu.make_async_copy(g, g, gsem).wait()
        pltpu.make_async_copy(h, h, hsem).wait()

    def stage_z():
        b = z * 4 + y
        send_chunk(mychip, c, zpeers, in_sem.at[b], inh_sem.at[b])

    def stage_y(z0):
        b = z0 * 4 + y

        @pl.when(z != z0)
        def _():
            wait_chunks(1, in_sem.at[b], inh_sem.at[b])
        send_chunk(chip(z0, y, x), c, ypeers, in_sem.at[b], inh_sem.at[b])

    def stage_x(b):
        y0 = lax.rem(b, 4)

        @pl.when(y != y0)
        def _():
            wait_chunks(1, in_sem.at[b], inh_sem.at[b])
        send_chunk(b * 4 + x, c, xpeers, x_sem.at[b], xh_sem.at[b])

    def stage_d(b):
        wait_chunks(3, x_sem.at[b], xh_sem.at[b])
        g = gb.at[pl.ds(b * 4, 4), c]
        h = hb.at[pl.ds(b * 4, 4), c]
        send(g, g, send_sem, d_sem.at[b], partner)
        send(h, h, sendh_sem, dh_sem.at[b], partner)

    def arrive(b):
        wait_chunks(4, d_sem.at[b], dh_sem.at[b])

    stage_z()
    for cp in weights:
        cp.wait()
    x2 = x8[0:2, :]
    for i in range(1, 4):
        x2 = jnp.where(lax.rem(me, 4) == i, x8[2 * i:2 * i + 2, :], x2)
    rowid = lax.broadcasted_iota(jnp.int32, (8, PC), 0)
    xpad = jnp.concatenate([x2, jnp.zeros((14, C), f32)], 0).astype(bf16)
    a0[...] = jnp.dot(xpad, win_ref[...], preferred_element_type=f32)[0:8]
    for s in range(3):
        for k in range(2):
            rs[s, k] = jnp.broadcast_to(x2[k:k + 1, :], (8, C))
    s_acc[...] = jnp.zeros_like(s_acc)
    fs0[...] = jnp.zeros_like(fs0)
    fs1[...] = jnp.zeros_like(fs1)
    XS = (xs0, xs1)
    FS = (fs0, fs1)
    zero = jnp.zeros((8, PC), f32)

    def hrows(blk, p):
        return hb[blk * 4 + p // 2, p % 2]

    def body(t, par, n, act, pre):
        off = n * CH
        fcur, fprev, xcur, xnext = FS[par], FS[1 - par], XS[par], XS[1 - par]
        pcol = pl.ds(pl.multiple_of(n * PC, PC), PC)

        def prefix(s, k):
            blk = t - 1 - LAG * s
            carry = rs[s, k, :, pcol]
            for p2 in range(J // 16):
                xr = []
                for p in (2 * p2, 2 * p2 + 1):
                    r0 = k * J + p * 8
                    v = fprev[s, pl.ds(r0, 8), pcol] * jnp.concatenate([hrows(blk, p)] * (PC // 128), 1)
                    fprev[s, pl.ds(r0, 8), pcol] = zero
                    cum = v
                    for sh in (1, 2, 4):
                        cum = cum + jnp.where(rowid >= sh, pltpu.roll(cum, sh, 0), 0.0)
                    xr.append(carry + (cum - v))
                    carry = carry + jnp.broadcast_to(cum[7:8, :], (8, PC))
                xnext[pl.ds((s * 2 + k) * J + p2 * 16, 16), pcol] = jnp.concatenate(xr, 0).astype(bf16)
            rs[s, k, :, pcol] = carry

        pieces = [(s, k) for s in pre for k in range(2)]
        mm = [s for s in act if s >= 1]
        outs = [s for s in act if s <= 2]
        slot = {s: lax.rem(t - LAG * s, RING) for s in act}
        G = [None] * NS
        acc = None

        def columns(i):
            return pl.ds(pl.multiple_of(off + i * SUB, SUB), SUB)

        def d1(i):
            lo, hi = (mm[0] - 1) * M, mm[-1] * M
            return jnp.dot(xcur[lo:hi, :], win_ref[:, columns(i)], preferred_element_type=f32)

        def gelus(i, A):
            cols = columns(i)
            gs = []
            for s in act:
                if s == 0:
                    chips = pl.ds(t * 4, 4)
                    g1 = gb[chips, :, 0, :, cols].astype(f32).reshape(J, SUB) * 0.5 + 0.5
                    b1 = gb[chips, :, 1, :, cols].astype(f32).reshape(J, SUB) * 0.5
                    g_ring[slot[0], :, cols] = g1
                    b_ring[slot[0], :, cols] = b1
                    for k in range(2):
                        gs.append(gelu_half(a0[k:k + 1, cols] * g1 + b1).astype(bf16))
                else:
                    g1 = g_ring[slot[s], :, cols]
                    b1 = b_ring[slot[s], :, cols]
                    base = (s - mm[0]) * M
                    for k in range(2):
                        ak = A[base + k * J: base + (k + 1) * J]
                        gv = gelu_half(ak * g1 + b1).astype(bf16)
                        if s <= 2:
                            gs.append(gv)
                        else:
                            blk = t - LAG * 3
                            tot = s_acc[k, :, cols]
                            for p in range(J // 8):
                                tot = tot + gv[p * 8:(p + 1) * 8].astype(f32) * jnp.concatenate([hrows(blk, p)] * (SUB // 128), 1)
                            s_acc[k, :, cols] = tot
            if outs:
                return jnp.concatenate(gs, 0) if len(gs) > 1 else gs[0]

        def d2(i):
            return jnp.dot(G[i], wout_ref[columns(i), :], preferred_element_type=f32)

        np_ = len(pieces)
        for i in range(NS):
            A = d1(i) if mm else None
            G[i] = gelus(i, A)
            if outs and i >= D2LAG:
                r = d2(i - D2LAG)
                acc = r if acc is None else acc + r
            for (s, k) in pieces[np_ * i // NS: np_ * (i + 1) // NS]:
                prefix(s, k)
        if outs:
            for i in range(NS - D2LAG, NS):
                r = d2(i)
                acc = r if acc is None else acc + r
            for q, s in enumerate(outs):
                fcur[s] += acc[q * M:(q + 1) * M]

    def sets(t):
        act = tuple(s for s in range(4) if 0 <= t - LAG * s < NB)
        pre = tuple(s for s in range(3) if 0 <= t - 1 - LAG * s < NB)
        return act, pre

    def when(cond, fn, arg):
        if isinstance(cond, bool):
            if cond:
                fn(arg)
        else:
            pl.when(cond)(lambda: fn(arg))

    def step(t, par, act, pre):
        when(t + 2 < NB, stage_x, t + 2)
        when(t + 1 < NB, stage_d, t + 1)
        when(t < NB, arrive, t)
        lax.fori_loop(0, NCH, lambda n, _: (body(t, par, n, act, pre), 0)[1], 0)

    stage_y(0)
    stage_x(0)
    stage_y(1)
    stage_x(1)
    stage_d(0)
    nsteps = NB + 3 * LAG
    t = 0
    while t < nsteps:
        e = t
        while e < nsteps and sets(e) == sets(t):
            e += 1
        act, pre = sets(t)
        if e - t >= 4:
            def pair(u, _, t=t, act=act, pre=pre):
                for q in range(2):
                    step(t + 2 * u + q, (t + q) % 2, act, pre)
                return 0
            lax.fori_loop(0, (e - t) // 2, pair, 0)
        else:
            for tt in range(t, e):
                if tt in (1, 3):
                    stage_y(2 + tt // 2)
                step(tt, tt % 2, act, pre)
        t = e

    st = jnp.concatenate([jnp.sum(s_acc[k], axis=0, keepdims=True) for k in range(2)], 0)
    h1 = st.astype(bf16).astype(f32)
    h2 = (st - h1).astype(bf16).astype(f32)
    h3 = st - h1 - h2
    lhs = jnp.concatenate([h1, h2, h3, jnp.zeros((10, D), f32)], 0).astype(bf16)
    o = jnp.dot(lhs, wout_ref[...], preferred_element_type=f32)
    yall[z, y, x, c] = x2 + (o[0:2] + (o[2:4] + o[4:6]))

    def ysend(ref, i, peers):
        for p in peers:
            send(ref, ref, ysend_sem, y_sem.at[i], p)

    def ywait(i, shape_ref):
        pltpu.make_async_copy(shape_ref, shape_ref, y_sem.at[i]).wait()

    ysend(yall.at[z, y, x, c], 0, xpeers)
    ywait(0, yall.at[0, 0, pl.ds(0, 3), 0])
    ysend(yall.at[z, y, :, c], 1, ypeers)
    ywait(1, yall.at[0, pl.ds(0, 3), :, 0])
    ysend(yall.at[z, :, :, c], 2, zpeers)
    ywait(2, yall.at[pl.ds(0, 3), :, :, 0])
    ysend(yall.at[:, :, :, c], 3, [partner])
    ywait(3, yall.at[:, :, :, 0])
    for zz in range(4):
        for yy in range(4):
            for x2_ in range(2):
                rows = [yall[zz, yy, x2_ * 2 + i // 2, i % 2] for i in range(4)]
                y_ref[pl.ds((zz * 4 + yy) * 16 + x2_ * 8, 8), :] = jnp.concatenate(rows, 0)

    def drain(ref, sem):
        for view in (ref.at[pl.ds(0, 63), 0], ref.at[:, 0]):
            pltpu.make_async_copy(view, view, sem).wait()
    drain(gb, send_sem)
    drain(hb, sendh_sem)
    for view in (yall.at[pl.ds(0, 3), :, :, 0], yall.at[0, pl.ds(0, 3), :, 0], yall.at[0, 0, pl.ds(0, 3), 0], yall.at[:, :, :, 0]):
        pltpu.make_async_copy(view, view, ysend_sem).wait()


def solution(mesh):
    V = pltpu.VMEM
    dma = pltpu.SemaphoreType.DMA
    run = pl.pallas_call(
        kernel,
        out_shape=jax.ShapeDtypeStruct((256, C), f32),
        in_specs=[pl.BlockSpec(memory_space=pl.ANY)] * 6,
        out_specs=pl.BlockSpec(memory_space=pltpu.VMEM),
        scratch_shapes=[
            V((64, 2, 2, 8, D), bf16), V((64, 2, 8, 128), f32), V((C, D), bf16), V((D, C), bf16), V((8, C), f32),
            V((RING, J, D), f32), V((RING, J, D), f32),
            V((3 * M, C), bf16), V((3 * M, C), bf16), V((3, M, C), f32), V((3, M, C), f32),
            V((8, D), f32), V((3, 2, 8, C), f32), V((2, 8, D), f32), V((4, 4, 4, 2, 2, C), f32),
            dma((6,)), dma, dma, dma((NB,)), dma((NB,)), dma((NB,)), dma((NB,)), dma((NB,)), dma((NB,)), dma, dma((4,)),
        ],
        compiler_params=pltpu.CompilerParams(vmem_limit_bytes=60 * 2**20, collective_id=0, has_side_effects=True),
    )

    def local_run(x_init, w_in, w_out, mod_gamma, mod_beta, step_size):
        hb = jnp.broadcast_to(step_size[:, None], (8, 128))
        y = run(x_init.reshape(256, C), w_in, w_out, mod_gamma, mod_beta, hb)
        return y.reshape(x_init.shape)

    return jax.shard_map(local_run, mesh=mesh, in_specs=(P("data", None, None), P(None, None), P(None, None), P("time", None), P("time", None), P("time")), out_specs=P("data", None, None), check_vma=False)
```

```python
import math

import jax
import jax.numpy as jnp
from jax import lax
from jax.experimental import pallas as pl
from jax.experimental.pallas import tpu as pltpu
from jax.sharding import PartitionSpec as P

C = 768
D = 3072
T = 1024
J = 64
CH = 1024
LAG = 2
D2LAG = 2
SUB = 256
NB = T // J
NCH = D // CH
NS = CH // SUB
PC = C // NCH
RING = 3 * LAG + 1
M = 2 * J
K0 = math.sqrt(2.0 / math.pi)
K1 = 2.0 * K0
K3 = 8.0 * 0.044715 * K0
f32 = jnp.float32
bf16 = jnp.bfloat16


def gelu_half(w):
    return w * jnp.tanh(w * (K1 + K3 * (w * w))) + w


def kernel(x_hbm, win_hbm, wout_hbm, gam_hbm, bet_hbm, h_smem, y_ref,
           gb, hb, win_ref, wout_ref, x8, g_ring, b_ring, xs0, xs1, fs0, fs1, a0, rs, s_acc, yall,
           local_sem, send_sem, sendh_sem, in_sem, inh_sem, x_sem, xh_sem, d_sem, dh_sem, ysend_sem, y_sem):
    me = lax.axis_index("time")
    c = lax.rem(me, 2)
    x = lax.rem(me // 2, 4)
    y = lax.rem(me // 8, 4)
    z = me // 32

    def peer(zz, yy, xx, cc):
        return {"time": ((zz * 4 + yy) * 4 + xx) * 2 + cc}

    def chip(zz, yy, xx):
        return (zz * 4 + yy) * 4 + xx

    mychip = chip(z, y, x)
    zpeers = [peer(lax.rem(z + d, 4), y, x, c) for d in (1, 3, 2)]
    ypeers = [peer(z, lax.rem(y + d, 4), x, c) for d in (1, 3, 2)]
    xpeers = [peer(z, y, lax.rem(x + d, 4), c) for d in (1, 3, 2)]
    partner = peer(z, y, x, 1 - c)

    for j in range(8):
        hb[mychip, c, j:j + 1, :] = jnp.full((1, 128), h_smem[j], f32)
    own = [pltpu.make_async_copy(gam_hbm, gb.at[mychip, c, 0], local_sem.at[0]),
           pltpu.make_async_copy(bet_hbm, gb.at[mychip, c, 1], local_sem.at[1]),
           ]
    weights = [pltpu.make_async_copy(x_hbm.at[pl.ds(pl.multiple_of((me // 4) * 8, 8), 8)], x8, local_sem.at[3]),
               pltpu.make_async_copy(win_hbm, win_ref, local_sem.at[4]),
               pltpu.make_async_copy(wout_hbm, wout_ref, local_sem.at[5])]
    for cp in own + weights:
        cp.start()

    barrier = pltpu.get_barrier_semaphore()
    for p in zpeers + ypeers + xpeers + [partner]:
        pl.semaphore_signal(barrier, inc=1, device_id=p, device_id_type=pl.DeviceIdType.MESH)
    pl.semaphore_wait(barrier, 10)
    for cp in own:
        cp.wait()

    def send(src, dst, ssem, rsem, dev):
        pltpu.make_async_remote_copy(src_ref=src, dst_ref=dst, send_sem=ssem, recv_sem=rsem,
                                     device_id=dev, device_id_type=pl.DeviceIdType.MESH).start()

    def send_chunk(q, cc, peers, gsem, hsem):
        for p in peers:
            send(gb.at[q, cc], gb.at[q, cc], send_sem, gsem, p)
            send(hb.at[q, cc], hb.at[q, cc], sendh_sem, hsem, p)

    def wait_chunks(n, gsem, hsem):
        g = gb.at[pl.ds(0, n), 0]
        h = hb.at[pl.ds(0, n), 0]
        pltpu.make_async_copy(g, g, gsem).wait()
        pltpu.make_async_copy(h, h, hsem).wait()

    def stage_z():
        b = z * 4 + y
        send_chunk(mychip, c, zpeers, in_sem.at[b], inh_sem.at[b])

    def stage_y(z0):
        b = z0 * 4 + y

        @pl.when(z != z0)
        def _():
            wait_chunks(1, in_sem.at[b], inh_sem.at[b])
        send_chunk(chip(z0, y, x), c, ypeers, in_sem.at[b], inh_sem.at[b])

    def stage_x(b):
        y0 = lax.rem(b, 4)

        @pl.when(y != y0)
        def _():
            wait_chunks(1, in_sem.at[b], inh_sem.at[b])
        send_chunk(b * 4 + x, c, xpeers, x_sem.at[b], xh_sem.at[b])

    def stage_d(b):
        wait_chunks(3, x_sem.at[b], xh_sem.at[b])
        g = gb.at[pl.ds(b * 4, 4), c]
        h = hb.at[pl.ds(b * 4, 4), c]
        send(g, g, send_sem, d_sem.at[b], partner)
        send(h, h, sendh_sem, dh_sem.at[b], partner)

    def arrive(b):
        wait_chunks(4, d_sem.at[b], dh_sem.at[b])

    stage_z()
    for cp in weights:
        cp.wait()
    x2 = x8[0:2, :]
    for i in range(1, 4):
        x2 = jnp.where(lax.rem(me, 4) == i, x8[2 * i:2 * i + 2, :], x2)
    rowid = lax.broadcasted_iota(jnp.int32, (8, 128), 0)
    xpad = jnp.concatenate([x2, jnp.zeros((14, C), f32)], 0).astype(bf16)
    a0[...] = jnp.dot(xpad, win_ref[...], preferred_element_type=f32)[0:8]
    for s in range(3):
        for k in range(2):
            rs[s, k] = jnp.broadcast_to(x2[k:k + 1, :], (8, C))
    s_acc[...] = jnp.zeros_like(s_acc)
    fs0[...] = jnp.zeros_like(fs0)
    fs1[...] = jnp.zeros_like(fs1)
    XS = (xs0, xs1)
    FS = (fs0, fs1)

    hflat = hb.reshape(T, 128)

    def hrows(blk, p):
        return hb[blk * 4 + p // 2, p % 2]

    def hstrided(blk, p):
        return hflat[pl.ds(pl.multiple_of(blk * J, J) + p, 8, stride=8), :]

    def body(t, par, n, act, pre):
        off = n * CH
        fcur, fprev, xcur, xnext = FS[par], FS[1 - par], XS[par], XS[1 - par]
        pcol = pl.ds(pl.multiple_of(n * PC, PC), PC)

        def prefix(s, k):
            blk = t - 1 - LAG * s
            for cc in range(PC // 128):
                lt = n * (PC // 128) + cc
                lane = pl.ds(pl.multiple_of(n * PC, PC) + cc * 128, 128)
                run = None
                before = []
                for p in range(8):
                    v = fprev[s, lt, pl.ds(k * J + p, 8, stride=8), :] * hstrided(blk, p)
                    before.append(run)
                    run = v if run is None else run + v
                cum = run
                for sh in (1, 2, 4):
                    cum = cum + jnp.where(rowid >= sh, pltpu.roll(cum, sh, 0), 0.0)
                carry = rs[s, k, :, lane]
                base = carry + (cum - run)
                rs[s, k, :, lane] = carry + jnp.broadcast_to(cum[7:8, :], (8, 128))
                for p in range(8):
                    fprev[s, lt, pl.ds(k * J + p, 8, stride=8), :] = base if p == 0 else base + before[p]
                xnext[pl.ds((s * 2 + k) * J, J), lane] = fprev[s, lt, pl.ds(k * J, J), :].astype(bf16)
                fprev[s, lt, pl.ds(k * J, J), :] = jnp.zeros((J, 128), f32)

        pieces = [(s, k) for s in pre for k in range(2)]
        mm = [s for s in act if s >= 1]
        outs = [s for s in act if s <= 2]
        slot = {s: lax.rem(t - LAG * s, RING) for s in act}
        G = [None] * NS
        acc = None

        def columns(i):
            return pl.ds(pl.multiple_of(off + i * SUB, SUB), SUB)

        def d1(i):
            lo, hi = (mm[0] - 1) * M, mm[-1] * M
            return jnp.dot(xcur[lo:hi, :], win_ref[:, columns(i)], preferred_element_type=f32)

        def gelus(i, A):
            cols = columns(i)
            gs = []
            for s in act:
                if s == 0:
                    chips = pl.ds(t * 4, 4)
                    g1 = gb[chips, :, 0, :, cols].astype(f32).reshape(J, SUB) * 0.5 + 0.5
                    b1 = gb[chips, :, 1, :, cols].astype(f32).reshape(J, SUB) * 0.5
                    g_ring[slot[0], :, cols] = g1
                    b_ring[slot[0], :, cols] = b1
                    for k in range(2):
                        gs.append(gelu_half(a0[k:k + 1, cols] * g1 + b1).astype(bf16))
                else:
                    g1 = g_ring[slot[s], :, cols]
                    b1 = b_ring[slot[s], :, cols]
                    base = (s - mm[0]) * M
                    for k in range(2):
                        ak = A[base + k * J: base + (k + 1) * J]
                        gv = gelu_half(ak * g1 + b1).astype(bf16)
                        if s <= 2:
                            gs.append(gv)
                        else:
                            blk = t - LAG * 3
                            tot = s_acc[k, :, cols]
                            for p in range(J // 8):
                                tot = tot + gv[p * 8:(p + 1) * 8].astype(f32) * jnp.concatenate([hrows(blk, p)] * (SUB // 128), 1)
                            s_acc[k, :, cols] = tot
            if outs:
                return jnp.concatenate(gs, 0) if len(gs) > 1 else gs[0]

        def d2(i):
            return jnp.dot(G[i], wout_ref[columns(i), :], preferred_element_type=f32)

        np_ = len(pieces)
        for i in range(NS):
            A = d1(i) if mm else None
            G[i] = gelus(i, A)
            if outs and i >= D2LAG:
                r = d2(i - D2LAG)
                acc = r if acc is None else acc + r
            for (s, k) in pieces[np_ * i // NS: np_ * (i + 1) // NS]:
                prefix(s, k)
        if outs:
            for i in range(NS - D2LAG, NS):
                r = d2(i)
                acc = r if acc is None else acc + r
            for q, s in enumerate(outs):
                for ct in range(C // 128):
                    fcur[s, ct] += acc[q * M:(q + 1) * M, ct * 128:(ct + 1) * 128]

    def sets(t):
        act = tuple(s for s in range(4) if 0 <= t - LAG * s < NB)
        pre = tuple(s for s in range(3) if 0 <= t - 1 - LAG * s < NB)
        return act, pre

    def when(cond, fn, arg):
        if isinstance(cond, bool):
            if cond:
                fn(arg)
        else:
            pl.when(cond)(lambda: fn(arg))

    def step(t, par, act, pre):
        when(t < NB, arrive, t)
        when(t + 4 < NB, stage_x, t + 4)

        def piece(n, _):
            def mid(arg):
                pl.when(n == 1)(lambda: stage_d(arg))
            when(t + 1 < NB, mid, t + 1)
            body(t, par, n, act, pre)
            return 0
        lax.fori_loop(0, NCH, piece, 0)

    stage_y(0)
    for b in range(4):
        stage_x(b)
    stage_y(1)
    stage_d(0)
    nsteps = NB + 3 * LAG
    t = 0
    while t < nsteps:
        e = t
        while e < nsteps and sets(e) == sets(t):
            e += 1
        act, pre = sets(t)
        if e - t >= 4:
            def pair(u, _, t=t, act=act, pre=pre):
                for q in range(2):
                    step(t + 2 * u + q, (t + q) % 2, act, pre)
                return 0
            lax.fori_loop(0, (e - t) // 2, pair, 0)
        else:
            for tt in range(t, e):
                if tt in (1, 3):
                    stage_y(2 + tt // 2)
                step(tt, tt % 2, act, pre)
        t = e

    st = jnp.concatenate([jnp.sum(s_acc[k], axis=0, keepdims=True) for k in range(2)], 0)
    h1 = st.astype(bf16).astype(f32)
    h2 = (st - h1).astype(bf16).astype(f32)
    h3 = st - h1 - h2
    lhs = jnp.concatenate([h1, h2, h3, jnp.zeros((10, D), f32)], 0).astype(bf16)
    o = jnp.dot(lhs, wout_ref[...], preferred_element_type=f32)
    yall[z, y, x, c] = x2 + (o[0:2] + (o[2:4] + o[4:6]))

    def ysend(ref, i, peers):
        for p in peers:
            send(ref, ref, ysend_sem, y_sem.at[i], p)

    def ywait(i, shape_ref):
        pltpu.make_async_copy(shape_ref, shape_ref, y_sem.at[i]).wait()

    ysend(yall.at[z, y, x, c], 0, xpeers)
    ywait(0, yall.at[0, 0, pl.ds(0, 3), 0])
    ysend(yall.at[z, y, :, c], 1, ypeers)
    ywait(1, yall.at[0, pl.ds(0, 3), :, 0])
    ysend(yall.at[z, :, :, c], 2, zpeers)
    ywait(2, yall.at[pl.ds(0, 3), :, :, 0])
    ysend(yall.at[:, :, :, c], 3, [partner])
    ywait(3, yall.at[:, :, :, 0])
    for zz in range(4):
        for yy in range(4):
            for x2_ in range(2):
                rows = [yall[zz, yy, x2_ * 2 + i // 2, i % 2] for i in range(4)]
                y_ref[pl.ds((zz * 4 + yy) * 16 + x2_ * 8, 8), :] = jnp.concatenate(rows, 0)

    def drain(ref, sem):
        for view in (ref.at[pl.ds(0, 63), 0], ref.at[:, 0]):
            pltpu.make_async_copy(view, view, sem).wait()
    drain(gb, send_sem)
    drain(hb, sendh_sem)
    for view in (yall.at[pl.ds(0, 3), :, :, 0], yall.at[0, pl.ds(0, 3), :, 0], yall.at[0, 0, pl.ds(0, 3), 0], yall.at[:, :, :, 0]):
        pltpu.make_async_copy(view, view, ysend_sem).wait()


def solution(mesh):
    V = pltpu.VMEM
    dma = pltpu.SemaphoreType.DMA
    run = pl.pallas_call(
        kernel,
        out_shape=jax.ShapeDtypeStruct((256, C), f32),
        in_specs=[pl.BlockSpec(memory_space=pl.ANY)] * 5 + [pl.BlockSpec(memory_space=pltpu.SMEM)],
        out_specs=pl.BlockSpec(memory_space=pltpu.VMEM),
        scratch_shapes=[
            V((64, 2, 2, 8, D), bf16), V((64, 2, 8, 128), f32), V((C, D), bf16), V((D, C), bf16), V((8, C), f32),
            V((RING, J, D), f32), V((RING, J, D), f32),
            V((3 * M, C), bf16), V((3 * M, C), bf16), V((3, C // 128, M, 128), f32), V((3, C // 128, M, 128), f32),
            V((8, D), f32), V((3, 2, 8, C), f32), V((2, 8, D), f32), V((4, 4, 4, 2, 2, C), f32),
            dma((6,)), dma, dma, dma((NB,)), dma((NB,)), dma((NB,)), dma((NB,)), dma((NB,)), dma((NB,)), dma, dma((4,)),
        ],
        compiler_params=pltpu.CompilerParams(vmem_limit_bytes=60 * 2**20, collective_id=0, has_side_effects=True),
    )

    def local_run(x_init, w_in, w_out, mod_gamma, mod_beta, step_size):
        y = run(x_init.reshape(256, C), w_in, w_out, mod_gamma, mod_beta, step_size)
        return y.reshape(x_init.shape)

    return jax.shard_map(local_run, mesh=mesh, in_specs=(P("data", None, None), P(None, None), P(None, None), P("time", None), P("time", None), P("time")), out_specs=P("data", None, None), check_vma=False)
```

```python
import math

import jax
import jax.numpy as jnp
from jax import lax
from jax.experimental import pallas as pl
from jax.experimental.pallas import tpu as pltpu
from jax.sharding import PartitionSpec as P

C = 768
D = 3072
T = 1024
J = 64
CH = 1024
LAG = 2
D2LAG = 2
SUB = 256
NB = T // J
NCH = D // CH
NS = CH // SUB
PC = C // NCH
RING = 3 * LAG + 1
M = 2 * J
K0 = math.sqrt(2.0 / math.pi)
K1 = 2.0 * K0
K3 = 8.0 * 0.044715 * K0
f32 = jnp.float32
bf16 = jnp.bfloat16


def gelu_half(w):
    return w * jnp.tanh(w * (K1 + K3 * (w * w))) + w


def kernel(x_hbm, win_hbm, wout_hbm, gam_hbm, bet_hbm, h_smem, y_ref,
           gb, hb, win_ref, wout_ref, x8, g_ring, b_ring, xs0, xs1, fs0, fs1, a0, rs, s_acc, yp0, yp1, yp2,
           local_sem, send_sem, sendh_sem, in_sem, inh_sem, x_sem, xh_sem, xr_sem, xrh_sem, d_sem, dh_sem, ysend_sem, y_sem):
    me = lax.axis_index("time")
    c = lax.rem(me, 2)
    x = lax.rem(me // 2, 4)
    y = lax.rem(me // 8, 4)
    z = me // 32

    def peer(zz, yy, xx, cc):
        return {"time": ((zz * 4 + yy) * 4 + xx) * 2 + cc}

    def chip(zz, yy, xx):
        return (zz * 4 + yy) * 4 + xx

    mychip = chip(z, y, x)
    zpeers = [peer(lax.rem(z + d, 4), y, x, c) for d in (1, 3, 2)]
    ypeers = [peer(z, lax.rem(y + d, 4), x, c) for d in (1, 3, 2)]
    xpeers = [peer(z, y, lax.rem(x + d, 4), c) for d in (1, 3, 2)]
    partner = peer(z, y, x, 1 - c)

    for j in range(8):
        hb[mychip, c, j:j + 1, :] = jnp.full((1, 128), h_smem[j], f32)
    own = [pltpu.make_async_copy(gam_hbm, gb.at[mychip, c, 0], local_sem.at[0]),
           pltpu.make_async_copy(bet_hbm, gb.at[mychip, c, 1], local_sem.at[1]),
           ]
    weights = [pltpu.make_async_copy(x_hbm.at[pl.ds(pl.multiple_of((me // 4) * 8, 8), 8)], x8, local_sem.at[3]),
               pltpu.make_async_copy(win_hbm, win_ref, local_sem.at[4]),
               pltpu.make_async_copy(wout_hbm, wout_ref, local_sem.at[5])]
    for cp in own + weights:
        cp.start()

    barrier = pltpu.get_barrier_semaphore()
    for p in zpeers + ypeers + xpeers + [partner]:
        pl.semaphore_signal(barrier, inc=1, device_id=p, device_id_type=pl.DeviceIdType.MESH)
    pl.semaphore_wait(barrier, 10)
    for cp in own:
        cp.wait()

    def send(src, dst, ssem, rsem, dev):
        pltpu.make_async_remote_copy(src_ref=src, dst_ref=dst, send_sem=ssem, recv_sem=rsem,
                                     device_id=dev, device_id_type=pl.DeviceIdType.MESH).start()

    def send_chunk(q, cc, peers, gsem, hsem):
        for p in peers:
            send(gb.at[q, cc], gb.at[q, cc], send_sem, gsem, p)
            send(hb.at[q, cc], hb.at[q, cc], sendh_sem, hsem, p)

    def wait_chunks(n, gsem, hsem):
        g = gb.at[pl.ds(0, n), 0]
        h = hb.at[pl.ds(0, n), 0]
        pltpu.make_async_copy(g, g, gsem).wait()
        pltpu.make_async_copy(h, h, hsem).wait()

    def stage_z():
        b = z * 4 + y
        send_chunk(mychip, c, zpeers, in_sem.at[b], inh_sem.at[b])

    def send_y(z0):
        b = z0 * 4 + y
        send_chunk(chip(z0, y, x), c, ypeers, in_sem.at[b], inh_sem.at[b])

    def stage_y(z0):
        b = z0 * 4 + y

        @pl.when(z != z0)
        def _():
            wait_chunks(1, in_sem.at[b], inh_sem.at[b])
        send_y(z0)

    def stage_x(b):
        y0 = lax.rem(b, 4)

        @pl.when(y != y0)
        def _():
            wait_chunks(1, in_sem.at[b], inh_sem.at[b])
        send_chunk(b * 4 + x, c, xpeers[:2], x_sem.at[b], xh_sem.at[b])

    def stage_r(b):
        wait_chunks(2, x_sem.at[b], xh_sem.at[b])
        right, left = xpeers[0], xpeers[1]
        ql, qr = b * 4 + lax.rem(x + 3, 4), b * 4 + lax.rem(x + 1, 4)
        send(gb.at[ql, c, 0], gb.at[ql, c, 0], send_sem, xr_sem.at[b], right)
        send(gb.at[qr, c, 1], gb.at[qr, c, 1], send_sem, xr_sem.at[b], left)
        send(hb.at[ql, c], hb.at[ql, c], sendh_sem, xrh_sem.at[b], right)

    def stage_d(b):
        wait_chunks(1, xr_sem.at[b], xrh_sem.at[b])
        g = gb.at[pl.ds(b * 4, 4), c]
        h = hb.at[pl.ds(b * 4, 4), c]
        send(g, g, send_sem, d_sem.at[b], partner)
        send(h, h, sendh_sem, dh_sem.at[b], partner)

    def arrive(b):
        wait_chunks(4, d_sem.at[b], dh_sem.at[b])

    pl.when(z == 0)(stage_z)

    @pl.when(z != 0)
    def _():
        wait_chunks(1, in_sem.at[y], inh_sem.at[y])
        stage_z()
    pl.when(y == 0)(lambda: send_y(0))
    stage_x(0)
    pl.when(y != 0)(lambda: send_y(0))
    stage_x(1)
    for cp in weights:
        cp.wait()
    x2 = x8[0:2, :]
    for i in range(1, 4):
        x2 = jnp.where(lax.rem(me, 4) == i, x8[2 * i:2 * i + 2, :], x2)
    rowid = lax.broadcasted_iota(jnp.int32, (8, 128), 0)
    xpad = jnp.concatenate([x2, jnp.zeros((14, C), f32)], 0).astype(bf16)
    a0[...] = jnp.dot(xpad, win_ref[...], preferred_element_type=f32)[0:8]
    for s in range(3):
        for k in range(2):
            rs[s, k] = jnp.broadcast_to(x2[k:k + 1, :], (8, C))
    s_acc[...] = jnp.zeros_like(s_acc)
    fs0[...] = jnp.zeros_like(fs0)
    fs1[...] = jnp.zeros_like(fs1)
    XS = (xs0, xs1)
    FS = (fs0, fs1)

    hflat = hb.reshape(T, 128)

    def hrows(blk, p):
        return hb[blk * 4 + p // 2, p % 2]

    def hstrided(blk, p):
        return hflat[pl.ds(pl.multiple_of(blk * J, J) + p, 8, stride=8), :]

    def body(t, par, n, act, pre):
        off = n * CH
        fcur, fprev, xcur, xnext = FS[par], FS[1 - par], XS[par], XS[1 - par]
        pcol = pl.ds(pl.multiple_of(n * PC, PC), PC)

        def prefix(s, k):
            blk = t - 1 - LAG * s
            for cc in range(PC // 128):
                lt = n * (PC // 128) + cc
                lane = pl.ds(pl.multiple_of(n * PC, PC) + cc * 128, 128)
                run = None
                before = []
                for p in range(8):
                    v = fprev[s, lt, pl.ds(k * J + p, 8, stride=8), :] * hstrided(blk, p)
                    before.append(run)
                    run = v if run is None else run + v
                cum = run
                for sh in (1, 2, 4):
                    cum = cum + jnp.where(rowid >= sh, pltpu.roll(cum, sh, 0), 0.0)
                carry = rs[s, k, :, lane]
                base = carry + (cum - run)
                rs[s, k, :, lane] = carry + jnp.broadcast_to(cum[7:8, :], (8, 128))
                for p in range(8):
                    fprev[s, lt, pl.ds(k * J + p, 8, stride=8), :] = base if p == 0 else base + before[p]
                xnext[pl.ds((s * 2 + k) * J, J), lane] = fprev[s, lt, pl.ds(k * J, J), :].astype(bf16)
                fprev[s, lt, pl.ds(k * J, J), :] = jnp.zeros((J, 128), f32)

        pieces = [(s, k) for s in pre for k in range(2)]
        mm = [s for s in act if s >= 1]
        outs = [s for s in act if s <= 2]
        slot = {s: lax.rem(t - LAG * s, RING) for s in act}
        G = [None] * NS
        acc = None

        def columns(i):
            return pl.ds(pl.multiple_of(off + i * SUB, SUB), SUB)

        def d1(i):
            lo, hi = (mm[0] - 1) * M, mm[-1] * M
            return jnp.dot(xcur[lo:hi, :], win_ref[:, columns(i)], preferred_element_type=f32)

        def gelus(i, A):
            cols = columns(i)
            gs = []
            for s in act:
                if s == 0:
                    chips = pl.ds(t * 4, 4)
                    g1 = gb[chips, :, 0, :, cols].astype(f32).reshape(J, SUB) * 0.5 + 0.5
                    b1 = gb[chips, :, 1, :, cols].astype(f32).reshape(J, SUB) * 0.5
                    g_ring[slot[0], :, cols] = g1
                    b_ring[slot[0], :, cols] = b1
                    for k in range(2):
                        gs.append(gelu_half(a0[k:k + 1, cols] * g1 + b1).astype(bf16))
                else:
                    g1 = g_ring[slot[s], :, cols]
                    b1 = b_ring[slot[s], :, cols]
                    base = (s - mm[0]) * M
                    for k in range(2):
                        ak = A[base + k * J: base + (k + 1) * J]
                        gv = gelu_half(ak * g1 + b1).astype(bf16)
                        if s <= 2:
                            gs.append(gv)
                        else:
                            blk = t - LAG * 3
                            tot = s_acc[k, :, cols]
                            for p in range(J // 8):
                                tot = tot + gv[p * 8:(p + 1) * 8].astype(f32) * jnp.concatenate([hrows(blk, p)] * (SUB // 128), 1)
                            s_acc[k, :, cols] = tot
            if outs:
                return jnp.concatenate(gs, 0) if len(gs) > 1 else gs[0]

        def d2(i):
            return jnp.dot(G[i], wout_ref[columns(i), :], preferred_element_type=f32)

        np_ = len(pieces)
        for i in range(NS):
            A = d1(i) if mm else None
            G[i] = gelus(i, A)
            if outs and i >= D2LAG:
                r = d2(i - D2LAG)
                acc = r if acc is None else acc + r
            for (s, k) in pieces[np_ * i // NS: np_ * (i + 1) // NS]:
                prefix(s, k)
        if outs:
            for i in range(NS - D2LAG, NS):
                r = d2(i)
                acc = r if acc is None else acc + r
            for q, s in enumerate(outs):
                for ct in range(C // 128):
                    fcur[s, ct] += acc[q * M:(q + 1) * M, ct * 128:(ct + 1) * 128]

    def sets(t):
        act = tuple(s for s in range(4) if 0 <= t - LAG * s < NB)
        pre = tuple(s for s in range(3) if 0 <= t - 1 - LAG * s < NB)
        return act, pre

    def when(cond, fn, arg):
        if isinstance(cond, bool):
            if cond:
                fn(arg)
        else:
            pl.when(cond)(lambda: fn(arg))

    def step(t, par, act, pre):
        when(t < NB, arrive, t)
        if isinstance(t, int) and t == 1:
            stage_x(4)

        def piece(n, _):
            def at(k, fn, arg):
                if isinstance(arg, int):
                    if arg < NB:
                        pl.when(n == k)(lambda: fn(arg))
                else:
                    pl.when(jnp.logical_and(n == k, arg < NB))(lambda: fn(arg))
            at(1, stage_r, t + 2)
            at(2, stage_d, t + 1)
            if not (isinstance(t, int) and t == 0):
                at(2, stage_x, t + 4)
            body(t, par, n, act, pre)
            return 0
        lax.fori_loop(0, NCH, piece, 0)

    stage_r(0)
    stage_x(2)
    stage_r(1)
    stage_d(0)
    stage_x(3)
    stage_y(1)
    nsteps = NB + 3 * LAG
    t = 0
    while t < nsteps:
        e = t
        while e < nsteps and sets(e) == sets(t):
            e += 1
        act, pre = sets(t)
        if e - t >= 4:
            def pair(u, _, t=t, act=act, pre=pre):
                for q in range(2):
                    step(t + 2 * u + q, (t + q) % 2, act, pre)
                return 0
            lax.fori_loop(0, (e - t) // 2, pair, 0)
        else:
            for tt in range(t, e):
                if tt in (1, 3):
                    stage_y(2 + tt // 2)
                step(tt, tt % 2, act, pre)
        t = e

    st = jnp.concatenate([jnp.sum(s_acc[k], axis=0, keepdims=True) for k in range(2)], 0)
    h1 = st.astype(bf16).astype(f32)
    h2 = (st - h1).astype(bf16).astype(f32)
    h3 = st - h1 - h2
    lhs = jnp.concatenate([h1, h2, h3, jnp.zeros((10, D), f32)], 0).astype(bf16)
    o = jnp.dot(lhs, wout_ref[...], preferred_element_type=f32)
    yv = x2 + (o[0:2] + (o[2:4] + o[4:6]))
    YP = (yp0, yp1, yp2)
    W = C // 3
    coords = (z, y, x)
    peers = (zpeers, ypeers, xpeers)
    views = (lambda r: r.at[0, 0, pl.ds(0, 3), 0], lambda r: r.at[0, pl.ds(0, 3), :, 0], lambda r: r.at[pl.ds(0, 3), :, :, 0], lambda r: r.at[:, :, :, 0])
    for p in range(3):
        YP[p][z, y, x, c] = yv[:, p * W:(p + 1) * W]

    def ywait(p, k):
        v = views[k](YP[p])
        pltpu.make_async_copy(v, v, y_sem.at[p, k]).wait()

    for k in range(4):
        for p in range(3):
            if k:
                ywait(p, k - 1)
            done = [(p + e) % 3 for e in range(k)]
            ref = YP[p].at[tuple(slice(None) if a in done else coords[a] for a in range(3)) + (c,)]
            for dev in (peers[(p + k) % 3] if k < 3 else [partner]):
                send(ref, ref, ysend_sem.at[p], y_sem.at[p, k], dev)
    for p in range(3):
        ywait(p, 3)
        for zz in range(4):
            for yy in range(4):
                for xx in (0, 2):
                    rows = [YP[p][zz, yy, xx + i // 2, i % 2] for i in range(4)]
                    y_ref[pl.ds((zz * 4 + yy) * 16 + xx * 4, 8), p * W:(p + 1) * W] = jnp.concatenate(rows, 0)

    def drain(ref, sem):
        for view in (ref.at[pl.ds(0, 63), 0], ref.at[:, 0]):
            pltpu.make_async_copy(view, view, sem).wait()
    drain(gb, send_sem)
    drain(hb, sendh_sem)
    for p in range(3):
        for view in views:
            v = view(YP[p])
            pltpu.make_async_copy(v, v, ysend_sem.at[p]).wait()


def solution(mesh):
    V = pltpu.VMEM
    dma = pltpu.SemaphoreType.DMA
    run = pl.pallas_call(
        kernel,
        out_shape=jax.ShapeDtypeStruct((256, C), f32),
        in_specs=[pl.BlockSpec(memory_space=pl.ANY)] * 5 + [pl.BlockSpec(memory_space=pltpu.SMEM)],
        out_specs=pl.BlockSpec(memory_space=pltpu.VMEM),
        scratch_shapes=[
            V((64, 2, 2, 8, D), bf16), V((64, 2, 8, 128), f32), V((C, D), bf16), V((D, C), bf16), V((8, C), f32),
            V((RING, J, D), f32), V((RING, J, D), f32),
            V((3 * M, C), bf16), V((3 * M, C), bf16), V((3, C // 128, M, 128), f32), V((3, C // 128, M, 128), f32),
            V((8, D), f32), V((3, 2, 8, C), f32), V((2, 8, D), f32), *[V((4, 4, 4, 2, 2, C // 3), f32) for _ in range(3)],
            dma((6,)), dma, dma, *[dma((NB,)) for _ in range(8)], dma((3,)), dma((3, 4)),
        ],
        compiler_params=pltpu.CompilerParams(vmem_limit_bytes=60 * 2**20, collective_id=0, has_side_effects=True),
    )

    def local_run(x_init, w_in, w_out, mod_gamma, mod_beta, step_size):
        y = run(x_init.reshape(256, C), w_in, w_out, mod_gamma, mod_beta, step_size)
        return y.reshape(x_init.shape)

    return jax.shard_map(local_run, mesh=mesh, in_specs=(P("data", None, None), P(None, None), P(None, None), P("time", None), P("time", None), P("time")), out_specs=P("data", None, None), check_vma=False)
```

```python
import math

import jax
import jax.numpy as jnp
from jax import lax
from jax.experimental import pallas as pl
from jax.experimental.pallas import tpu as pltpu
from jax.sharding import PartitionSpec as P

C = 768
D = 3072
T = 1024
J = 64
CH = 1024
LAG = 2
D2LAG = 2
SUB = 256
NB = T // J
NCH = D // CH
NS = CH // SUB
PC = C // NCH
RING = 3 * LAG + 1
M = 2 * J
K0 = math.sqrt(2.0 / math.pi)
K1 = 2.0 * K0
K3 = 8.0 * 0.044715 * K0
f32 = jnp.float32
bf16 = jnp.bfloat16


def gelu_half(w):
    return w * jnp.tanh(w * (K1 + K3 * (w * w))) + w


def kernel(x_hbm, win_hbm, wout_hbm, gam_hbm, bet_hbm, h_smem, y_ref,
           gb, hb, win_ref, wout_ref, x8, g_ring, b_ring, xs0, xs1, fs0, fs1, a0, rs, s_acc, yp0, yp1, yp2,
           local_sem, send_sem, sendh_sem, in_sem, inh_sem, x_sem, xh_sem, xr_sem, xrh_sem, d_sem, dh_sem, ysend_sem, y_sem):
    me = lax.axis_index("time")
    c = lax.rem(me, 2)
    x = lax.rem(me // 2, 4)
    y = lax.rem(me // 8, 4)
    z = me // 32

    def peer(zz, yy, xx, cc):
        return {"time": ((zz * 4 + yy) * 4 + xx) * 2 + cc}

    def chip(zz, yy, xx):
        return (zz * 4 + yy) * 4 + xx

    mychip = chip(z, y, x)
    zpeers = [peer(lax.rem(z + d, 4), y, x, c) for d in (2, 1, 3)]
    ypeers = [peer(z, lax.rem(y + d, 4), x, c) for d in (2, 1, 3)]
    xpeers = [peer(z, y, lax.rem(x + d, 4), c) for d in (1, 3, 2)]
    partner = peer(z, y, x, 1 - c)

    for j in range(8):
        hb[mychip, c, j:j + 1, :] = jnp.full((1, 128), h_smem[j], f32)
    own = [pltpu.make_async_copy(gam_hbm, gb.at[mychip, c, 0], local_sem.at[0]),
           pltpu.make_async_copy(bet_hbm, gb.at[mychip, c, 1], local_sem.at[1]),
           ]
    weights = [pltpu.make_async_copy(x_hbm.at[pl.ds(pl.multiple_of((me // 4) * 8, 8), 8)], x8, local_sem.at[3]),
               pltpu.make_async_copy(win_hbm, win_ref, local_sem.at[4]),
               pltpu.make_async_copy(wout_hbm, wout_ref, local_sem.at[5])]
    for cp in own + weights:
        cp.start()

    barrier = pltpu.get_barrier_semaphore()
    for p in zpeers + ypeers + xpeers + [partner]:
        pl.semaphore_signal(barrier, inc=1, device_id=p, device_id_type=pl.DeviceIdType.MESH)
    pl.semaphore_wait(barrier, 10)
    for cp in own:
        cp.wait()

    def send(src, dst, ssem, rsem, dev):
        pltpu.make_async_remote_copy(src_ref=src, dst_ref=dst, send_sem=ssem, recv_sem=rsem,
                                     device_id=dev, device_id_type=pl.DeviceIdType.MESH).start()

    def send_part(q, a, peers, gsem, hsem):
        for p in peers:
            send(gb.at[q, c, a], gb.at[q, c, a], send_sem, gsem, p)
            if a == 0:
                send(hb.at[q, c], hb.at[q, c], sendh_sem, hsem, p)

    def wait_part(n, a, gsem, hsem):
        g = gb.at[pl.ds(0, n), 0, 0]
        pltpu.make_async_copy(g, g, gsem).wait()
        if a == 0:
            h = hb.at[pl.ds(0, n), 0]
            pltpu.make_async_copy(h, h, hsem).wait()

    def wait_in(b, a):
        wait_part(1, a, in_sem.at[a, b], inh_sem.at[b])

    def stage_z():
        b = z * 4 + y
        for a in range(2):
            send_part(mychip, a, zpeers, in_sem.at[a, b], inh_sem.at[b])

    def send_y(z0, a):
        b = z0 * 4 + y
        send_part(chip(z0, y, x), a, ypeers, in_sem.at[a, b], inh_sem.at[b])

    def stage_y(z0):
        for a in range(2):
            pl.when(z != z0)(lambda a=a: wait_in(z0 * 4 + y, a))
            send_y(z0, a)

    def part_x(b, a):
        pl.when(y != lax.rem(b, 4))(lambda: wait_in(b, a))
        send_part(b * 4 + x, a, xpeers[:2], x_sem.at[a, b], xh_sem.at[b])

    def stage_x(b):
        for a in range(2):
            part_x(b, a)

    def part_r(b, a):
        wait_part(2, a, x_sem.at[a, b], xh_sem.at[b])
        if a == 0:
            send_part(b * 4 + lax.rem(x + 3, 4), 0, [xpeers[0]], xr_sem.at[0, b], xrh_sem.at[b])
        else:
            send_part(b * 4 + lax.rem(x + 1, 4), 1, [xpeers[1]], xr_sem.at[1, b], xrh_sem.at[b])

    def stage_r(b):
        for a in range(2):
            part_r(b, a)

    def part_d(b, a):
        wait_part(1, a, xr_sem.at[a, b], xrh_sem.at[b])
        g = gb.at[pl.ds(b * 4, 4), c, a]
        send(g, g, send_sem, d_sem.at[a, b], partner)
        if a == 0:
            h = hb.at[pl.ds(b * 4, 4), c]
            send(h, h, sendh_sem, dh_sem.at[b], partner)

    def stage_d(b):
        for a in range(2):
            part_d(b, a)

    def arrive(b):
        for a in range(2):
            wait_part(4, a, d_sem.at[a, b], dh_sem.at[b])

    pl.when(z == 0)(stage_z)
    for a in range(2):
        pl.when(z != 0)(lambda a=a: wait_in(y, a))
        send_y(0, a)
    pl.when(z != 0)(stage_z)
    part_x(0, 0)
    part_x(1, 0)
    part_x(0, 1)
    for cp in weights:
        cp.wait()
    x2 = x8[0:2, :]
    for i in range(1, 4):
        x2 = jnp.where(lax.rem(me, 4) == i, x8[2 * i:2 * i + 2, :], x2)
    rowid = lax.broadcasted_iota(jnp.int32, (8, 128), 0)
    xpad = jnp.concatenate([x2, jnp.zeros((14, C), f32)], 0).astype(bf16)
    a0[...] = jnp.dot(xpad, win_ref[...], preferred_element_type=f32)[0:8]
    for s in range(3):
        for k in range(2):
            rs[s, k] = jnp.broadcast_to(x2[k:k + 1, :], (8, C))
    s_acc[...] = jnp.zeros_like(s_acc)
    fs0[...] = jnp.zeros_like(fs0)
    fs1[...] = jnp.zeros_like(fs1)
    XS = (xs0, xs1)
    FS = (fs0, fs1)

    hflat = hb.reshape(T, 128)

    def hrows(blk, p):
        return hb[blk * 4 + p // 2, p % 2]

    def hstrided(blk, p):
        return hflat[pl.ds(pl.multiple_of(blk * J, J) + p, 8, stride=8), :]

    def body(t, par, n, act, pre):
        off = n * CH
        fcur, fprev, xcur, xnext = FS[par], FS[1 - par], XS[par], XS[1 - par]
        pcol = pl.ds(pl.multiple_of(n * PC, PC), PC)

        def prefix(s, k):
            blk = t - 1 - LAG * s
            for cc in range(PC // 128):
                lt = n * (PC // 128) + cc
                lane = pl.ds(pl.multiple_of(n * PC, PC) + cc * 128, 128)
                run = None
                before = []
                for p in range(8):
                    v = fprev[s, lt, pl.ds(k * J + p, 8, stride=8), :] * hstrided(blk, p)
                    before.append(run)
                    run = v if run is None else run + v
                cum = run
                for sh in (1, 2, 4):
                    cum = cum + jnp.where(rowid >= sh, pltpu.roll(cum, sh, 0), 0.0)
                carry = rs[s, k, :, lane]
                base = carry + (cum - run)
                rs[s, k, :, lane] = carry + jnp.broadcast_to(cum[7:8, :], (8, 128))
                for p in range(8):
                    fprev[s, lt, pl.ds(k * J + p, 8, stride=8), :] = base if p == 0 else base + before[p]
                xnext[pl.ds((s * 2 + k) * J, J), lane] = fprev[s, lt, pl.ds(k * J, J), :].astype(bf16)
                fprev[s, lt, pl.ds(k * J, J), :] = jnp.zeros((J, 128), f32)

        pieces = [(s, k) for s in pre for k in range(2)]
        mm = [s for s in act if s >= 1]
        outs = [s for s in act if s <= 2]
        slot = {s: lax.rem(t - LAG * s, RING) for s in act}
        G = [None] * NS
        acc = None

        def columns(i):
            return pl.ds(pl.multiple_of(off + i * SUB, SUB), SUB)

        def d1(i):
            lo, hi = (mm[0] - 1) * M, mm[-1] * M
            return jnp.dot(xcur[lo:hi, :], win_ref[:, columns(i)], preferred_element_type=f32)

        def gelus(i, A):
            cols = columns(i)
            gs = []
            for s in act:
                if s == 0:
                    chips = pl.ds(t * 4, 4)
                    g1 = gb[chips, :, 0, :, cols].astype(f32).reshape(J, SUB) * 0.5 + 0.5
                    b1 = gb[chips, :, 1, :, cols].astype(f32).reshape(J, SUB) * 0.5
                    g_ring[slot[0], :, cols] = g1
                    b_ring[slot[0], :, cols] = b1
                    for k in range(2):
                        gs.append(gelu_half(a0[k:k + 1, cols] * g1 + b1).astype(bf16))
                else:
                    g1 = g_ring[slot[s], :, cols]
                    b1 = b_ring[slot[s], :, cols]
                    base = (s - mm[0]) * M
                    for k in range(2):
                        ak = A[base + k * J: base + (k + 1) * J]
                        gv = gelu_half(ak * g1 + b1).astype(bf16)
                        if s <= 2:
                            gs.append(gv)
                        else:
                            blk = t - LAG * 3
                            tot = s_acc[k, :, cols]
                            for p in range(J // 8):
                                tot = tot + gv[p * 8:(p + 1) * 8].astype(f32) * jnp.concatenate([hrows(blk, p)] * (SUB // 128), 1)
                            s_acc[k, :, cols] = tot
            if outs:
                return jnp.concatenate(gs, 0) if len(gs) > 1 else gs[0]

        def d2(i):
            return jnp.dot(G[i], wout_ref[columns(i), :], preferred_element_type=f32)

        np_ = len(pieces)
        for i in range(NS):
            A = d1(i) if mm else None
            G[i] = gelus(i, A)
            if outs and i >= D2LAG:
                r = d2(i - D2LAG)
                acc = r if acc is None else acc + r
            for (s, k) in pieces[np_ * i // NS: np_ * (i + 1) // NS]:
                prefix(s, k)
        if outs:
            for i in range(NS - D2LAG, NS):
                r = d2(i)
                acc = r if acc is None else acc + r
            for q, s in enumerate(outs):
                for ct in range(C // 128):
                    fcur[s, ct] += acc[q * M:(q + 1) * M, ct * 128:(ct + 1) * 128]

    def sets(t):
        act = tuple(s for s in range(4) if 0 <= t - LAG * s < NB)
        pre = tuple(s for s in range(3) if 0 <= t - 1 - LAG * s < NB)
        return act, pre

    def when(cond, fn, arg):
        if isinstance(cond, bool):
            if cond:
                fn(arg)
        else:
            pl.when(cond)(lambda: fn(arg))

    def step(t, par, act, pre):
        when(t < NB, arrive, t)
        if isinstance(t, int) and t == 1:
            stage_x(4)

        def piece(n, _):
            def at(k, fn, arg):
                if isinstance(arg, int):
                    if arg < NB:
                        pl.when(n == k)(lambda: fn(arg))
                else:
                    pl.when(jnp.logical_and(n == k, arg < NB))(lambda: fn(arg))
            at(1, stage_r, t + 2)
            at(2, stage_d, t + 1)
            if not (isinstance(t, int) and t == 0):
                at(2, stage_x, t + 4)
            body(t, par, n, act, pre)
            return 0
        lax.fori_loop(0, NCH, piece, 0)

    part_r(0, 0)
    part_x(1, 1)
    part_r(0, 1)
    part_d(0, 0)
    part_r(1, 0)
    stage_x(2)
    part_d(0, 1)
    part_r(1, 1)
    stage_y(1)
    stage_x(3)
    nsteps = NB + 3 * LAG
    t = 0
    while t < nsteps:
        e = t
        while e < nsteps and sets(e) == sets(t):
            e += 1
        act, pre = sets(t)
        if e - t >= 4:
            def pair(u, _, t=t, act=act, pre=pre):
                for q in range(2):
                    step(t + 2 * u + q, (t + q) % 2, act, pre)
                return 0
            lax.fori_loop(0, (e - t) // 2, pair, 0)
        else:
            for tt in range(t, e):
                if tt in (1, 3):
                    stage_y(2 + tt // 2)
                step(tt, tt % 2, act, pre)
        t = e

    st = jnp.concatenate([jnp.sum(s_acc[k], axis=0, keepdims=True) for k in range(2)], 0)
    h1 = st.astype(bf16).astype(f32)
    h2 = (st - h1).astype(bf16).astype(f32)
    h3 = st - h1 - h2
    lhs = jnp.concatenate([h1, h2, h3, jnp.zeros((10, D), f32)], 0).astype(bf16)
    o = jnp.dot(lhs, wout_ref[...], preferred_element_type=f32)
    yv = x2 + (o[0:2] + (o[2:4] + o[4:6]))
    YP = (yp0, yp1, yp2)
    W = C // 3
    coords = (z, y, x)
    peers = (zpeers, ypeers, [xpeers[2], xpeers[0], xpeers[1]])
    views = (lambda r: r.at[0, 0, pl.ds(0, 3), 0], lambda r: r.at[0, pl.ds(0, 3), :, 0], lambda r: r.at[pl.ds(0, 3), :, :, 0], lambda r: r.at[:, :, :, 0])
    for p in range(3):
        YP[p][z, y, x, c] = yv[:, p * W:(p + 1) * W]

    def ywait(p, k):
        v = views[k](YP[p])
        pltpu.make_async_copy(v, v, y_sem.at[p, k]).wait()

    for k in range(4):
        for p in range(3):
            if k:
                ywait(p, k - 1)
            done = [(p + e) % 3 for e in range(k)]
            ref = YP[p].at[tuple(slice(None) if a in done else coords[a] for a in range(3)) + (c,)]
            for dev in (peers[(p + k) % 3] if k < 3 else [partner]):
                send(ref, ref, ysend_sem.at[p], y_sem.at[p, k], dev)
    for p in range(3):
        ywait(p, 3)
        for zz in range(4):
            for yy in range(4):
                for xx in (0, 2):
                    rows = [YP[p][zz, yy, xx + i // 2, i % 2] for i in range(4)]
                    y_ref[pl.ds((zz * 4 + yy) * 16 + xx * 4, 8), p * W:(p + 1) * W] = jnp.concatenate(rows, 0)

    def drain(ref, sem):
        for view in (ref.at[pl.ds(0, 63), 0], ref.at[:, 0]):
            pltpu.make_async_copy(view, view, sem).wait()
    drain(gb, send_sem)
    drain(hb, sendh_sem)
    for p in range(3):
        for view in views:
            v = view(YP[p])
            pltpu.make_async_copy(v, v, ysend_sem.at[p]).wait()


def solution(mesh):
    V = pltpu.VMEM
    dma = pltpu.SemaphoreType.DMA
    run = pl.pallas_call(
        kernel,
        out_shape=jax.ShapeDtypeStruct((256, C), f32),
        in_specs=[pl.BlockSpec(memory_space=pl.ANY)] * 5 + [pl.BlockSpec(memory_space=pltpu.SMEM)],
        out_specs=pl.BlockSpec(memory_space=pltpu.VMEM),
        scratch_shapes=[
            V((64, 2, 2, 8, D), bf16), V((64, 2, 8, 128), f32), V((C, D), bf16), V((D, C), bf16), V((8, C), f32),
            V((RING, J, D), f32), V((RING, J, D), f32),
            V((3 * M, C), bf16), V((3 * M, C), bf16), V((3, C // 128, M, 128), f32), V((3, C // 128, M, 128), f32),
            V((8, D), f32), V((3, 2, 8, C), f32), V((2, 8, D), f32), *[V((4, 4, 4, 2, 2, C // 3), f32) for _ in range(3)],
            dma((6,)), dma, dma, *[dma(n) for _ in range(4) for n in ((2, NB), (NB,))], dma((3,)), dma((3, 4)),
        ],
        compiler_params=pltpu.CompilerParams(vmem_limit_bytes=60 * 2**20, collective_id=0, has_side_effects=True),
    )

    def local_run(x_init, w_in, w_out, mod_gamma, mod_beta, step_size):
        y = run(x_init.reshape(256, C), w_in, w_out, mod_gamma, mod_beta, step_size)
        return y.reshape(x_init.shape)

    return jax.shard_map(local_run, mesh=mesh, in_specs=(P("data", None, None), P(None, None), P(None, None), P("time", None), P("time", None), P("time")), out_specs=P("data", None, None), check_vma=False)
```

```python
import math

import jax
import jax.numpy as jnp
from jax import lax
from jax.experimental import pallas as pl
from jax.experimental.pallas import tpu as pltpu
from jax.sharding import PartitionSpec as P

C = 768
D = 3072
T = 1024
J = 64
CH = 1024
LAG = 2
D2LAG = 2
SUB = 256
NB = T // J
NCH = D // CH
NS = CH // SUB
PC = C // NCH
RING = 3 * LAG + 1
M = 2 * J
K0 = math.sqrt(2.0 / math.pi)
K1 = 2.0 * K0
K3 = 8.0 * 0.044715 * K0
f32 = jnp.float32
bf16 = jnp.bfloat16


def gelu_half(w):
    return w * jnp.tanh(w * (K1 + K3 * (w * w))) + w


def kernel(x_hbm, win_hbm, wout_hbm, gam_hbm, bet_hbm, h_smem, y_ref,
           gb, hb, win_ref, wout_ref, x8, g_ring, b_ring, xs0, xs1, fs0, fs1, a0, rs, s_acc, yp0, yp1, yp2,
           local_sem, send_sem, sendh_sem, in_sem, inh_sem, x_sem, xh_sem, xr_sem, xrh_sem, d_sem, dh_sem, ysend_sem, y_sem):
    me = lax.axis_index("time")
    c = lax.rem(me, 2)
    x = lax.rem(me // 2, 4)
    y = lax.rem(me // 8, 4)
    z = me // 32

    def peer(zz, yy, xx, cc):
        return {"time": ((zz * 4 + yy) * 4 + xx) * 2 + cc}

    def chip(zz, yy, xx):
        return (zz * 4 + yy) * 4 + xx

    mychip = chip(z, y, x)
    zpeers = [peer(lax.rem(z + d, 4), y, x, c) for d in (2, 1, 3)]
    ypeers = [peer(z, lax.rem(y + d, 4), x, c) for d in (2, 1, 3)]
    xpeers = [peer(z, y, lax.rem(x + d, 4), c) for d in (1, 3, 2)]
    partner = peer(z, y, x, 1 - c)

    for j in range(8):
        hb[mychip, c, j:j + 1, :] = jnp.full((1, 128), h_smem[j], f32)
    own = [pltpu.make_async_copy(gam_hbm, gb.at[mychip, c, 0], local_sem.at[0]),
           pltpu.make_async_copy(bet_hbm, gb.at[mychip, c, 1], local_sem.at[1]),
           ]
    weights = [pltpu.make_async_copy(x_hbm.at[pl.ds(pl.multiple_of((me // 4) * 8, 8), 8)], x8, local_sem.at[3]),
               pltpu.make_async_copy(win_hbm, win_ref, local_sem.at[4]),
               pltpu.make_async_copy(wout_hbm, wout_ref, local_sem.at[5])]
    for cp in own + weights:
        cp.start()

    barrier = pltpu.get_barrier_semaphore()
    for p in zpeers + ypeers + xpeers + [partner]:
        pl.semaphore_signal(barrier, inc=1, device_id=p, device_id_type=pl.DeviceIdType.MESH)
    pl.semaphore_wait(barrier, 10)
    for cp in own:
        cp.wait()

    def send(src, dst, ssem, rsem, dev):
        pltpu.make_async_remote_copy(src_ref=src, dst_ref=dst, send_sem=ssem, recv_sem=rsem,
                                     device_id=dev, device_id_type=pl.DeviceIdType.MESH).start()

    def send_part(q, a, peers, gsem, hsem):
        for p in peers:
            send(gb.at[q, c, a], gb.at[q, c, a], send_sem, gsem, p)
            if a == 0:
                send(hb.at[q, c], hb.at[q, c], sendh_sem, hsem, p)

    def wait_part(n, a, gsem, hsem):
        g = gb.at[pl.ds(0, n), 0, 0]
        pltpu.make_async_copy(g, g, gsem).wait()
        if a == 0:
            h = hb.at[pl.ds(0, n), 0]
            pltpu.make_async_copy(h, h, hsem).wait()

    def wait_in(b, a):
        wait_part(1, a, in_sem.at[a, b], inh_sem.at[b])

    def stage_z():
        b = z * 4 + y
        for a in range(2):
            send_part(mychip, a, zpeers, in_sem.at[a, b], inh_sem.at[b])

    def send_y(z0, a):
        b = z0 * 4 + y
        send_part(chip(z0, y, x), a, ypeers, in_sem.at[a, b], inh_sem.at[b])

    def stage_y(z0):
        for a in range(2):
            pl.when(z != z0)(lambda a=a: wait_in(z0 * 4 + y, a))
            send_y(z0, a)

    def part_x(b, a):
        pl.when(y != lax.rem(b, 4))(lambda: wait_in(b, a))
        send_part(b * 4 + x, a, xpeers[:2], x_sem.at[a, b], xh_sem.at[b])

    def stage_x(b):
        for a in range(2):
            part_x(b, a)

    def part_r(b, a):
        wait_part(2, a, x_sem.at[a, b], xh_sem.at[b])
        if a == 0:
            send_part(b * 4 + lax.rem(x + 3, 4), 0, [xpeers[0]], xr_sem.at[0, b], xrh_sem.at[b])
        else:
            send_part(b * 4 + lax.rem(x + 1, 4), 1, [xpeers[1]], xr_sem.at[1, b], xrh_sem.at[b])
        for e in (0, 1, 3):
            send_part(b * 4 + lax.rem(x + e, 4), a, [partner], d_sem.at[a, b], dh_sem.at[b])

    def stage_r(b):
        for a in range(2):
            part_r(b, a)

    def part_d(b, a):
        wait_part(1, a, xr_sem.at[a, b], xrh_sem.at[b])
        send_part(b * 4 + lax.rem(x + 2, 4), a, [partner], d_sem.at[a, b], dh_sem.at[b])

    def stage_d(b):
        for a in range(2):
            part_d(b, a)

    def arrive(b):
        for a in range(2):
            wait_part(4, a, d_sem.at[a, b], dh_sem.at[b])

    pl.when(z == 0)(stage_z)
    for a in range(2):
        pl.when(z != 0)(lambda a=a: wait_in(y, a))
        send_y(0, a)
    pl.when(z != 0)(stage_z)
    part_x(0, 0)
    part_x(1, 0)
    part_x(0, 1)
    for cp in weights:
        cp.wait()
    x2 = x8[0:2, :]
    for i in range(1, 4):
        x2 = jnp.where(lax.rem(me, 4) == i, x8[2 * i:2 * i + 2, :], x2)
    rowid = lax.broadcasted_iota(jnp.int32, (8, 128), 0)
    xpad = jnp.concatenate([x2, jnp.zeros((14, C), f32)], 0).astype(bf16)
    a0[...] = jnp.dot(xpad, win_ref[...], preferred_element_type=f32)[0:8]
    for s in range(3):
        for k in range(2):
            rs[s, k] = jnp.broadcast_to(x2[k:k + 1, :], (8, C))
    s_acc[...] = jnp.zeros_like(s_acc)
    fs0[...] = jnp.zeros_like(fs0)
    fs1[...] = jnp.zeros_like(fs1)
    XS = (xs0, xs1)
    FS = (fs0, fs1)

    hflat = hb.reshape(T, 128)

    def hrows(blk, p):
        return hb[blk * 4 + p // 2, p % 2]

    def hstrided(blk, p):
        return hflat[pl.ds(pl.multiple_of(blk * J, J) + p, 8, stride=8), :]

    def body(t, par, n, act, pre):
        off = n * CH
        fcur, fprev, xcur, xnext = FS[par], FS[1 - par], XS[par], XS[1 - par]
        pcol = pl.ds(pl.multiple_of(n * PC, PC), PC)

        def prefix(s, k):
            blk = t - 1 - LAG * s
            for cc in range(PC // 128):
                lt = n * (PC // 128) + cc
                lane = pl.ds(pl.multiple_of(n * PC, PC) + cc * 128, 128)
                run = None
                before = []
                for p in range(8):
                    v = fprev[s, lt, pl.ds(k * J + p, 8, stride=8), :] * hstrided(blk, p)
                    before.append(run)
                    run = v if run is None else run + v
                cum = run
                for sh in (1, 2, 4):
                    cum = cum + jnp.where(rowid >= sh, pltpu.roll(cum, sh, 0), 0.0)
                carry = rs[s, k, :, lane]
                base = carry + (cum - run)
                rs[s, k, :, lane] = carry + jnp.broadcast_to(cum[7:8, :], (8, 128))
                for p in range(8):
                    fprev[s, lt, pl.ds(k * J + p, 8, stride=8), :] = base if p == 0 else base + before[p]
                xnext[pl.ds((s * 2 + k) * J, J), lane] = fprev[s, lt, pl.ds(k * J, J), :].astype(bf16)
                fprev[s, lt, pl.ds(k * J, J), :] = jnp.zeros((J, 128), f32)

        pieces = [(s, k) for s in pre for k in range(2)]
        mm = [s for s in act if s >= 1]
        outs = [s for s in act if s <= 2]
        slot = {s: lax.rem(t - LAG * s, RING) for s in act}
        G = [None] * NS
        acc = None

        def columns(i):
            return pl.ds(pl.multiple_of(off + i * SUB, SUB), SUB)

        def d1(i):
            lo, hi = (mm[0] - 1) * M, mm[-1] * M
            return jnp.dot(xcur[lo:hi, :], win_ref[:, columns(i)], preferred_element_type=f32)

        def gelus(i, A):
            cols = columns(i)
            gs = []
            for s in act:
                if s == 0:
                    chips = pl.ds(t * 4, 4)
                    g1 = gb[chips, :, 0, :, cols].astype(f32).reshape(J, SUB) * 0.5 + 0.5
                    b1 = gb[chips, :, 1, :, cols].astype(f32).reshape(J, SUB) * 0.5
                    g_ring[slot[0], :, cols] = g1
                    b_ring[slot[0], :, cols] = b1
                    for k in range(2):
                        gs.append(gelu_half(a0[k:k + 1, cols] * g1 + b1).astype(bf16))
                else:
                    g1 = g_ring[slot[s], :, cols]
                    b1 = b_ring[slot[s], :, cols]
                    base = (s - mm[0]) * M
                    for k in range(2):
                        ak = A[base + k * J: base + (k + 1) * J]
                        gv = gelu_half(ak * g1 + b1).astype(bf16)
                        if s <= 2:
                            gs.append(gv)
                        else:
                            blk = t - LAG * 3
                            tot = s_acc[k, :, cols]
                            for p in range(J // 8):
                                tot = tot + gv[p * 8:(p + 1) * 8].astype(f32) * jnp.concatenate([hrows(blk, p)] * (SUB // 128), 1)
                            s_acc[k, :, cols] = tot
            if outs:
                return jnp.concatenate(gs, 0) if len(gs) > 1 else gs[0]

        def d2(i):
            return jnp.dot(G[i], wout_ref[columns(i), :], preferred_element_type=f32)

        np_ = len(pieces)
        for i in range(NS):
            A = d1(i) if mm else None
            G[i] = gelus(i, A)
            if outs and i >= D2LAG:
                r = d2(i - D2LAG)
                acc = r if acc is None else acc + r
            for (s, k) in pieces[np_ * i // NS: np_ * (i + 1) // NS]:
                prefix(s, k)
        if outs:
            for i in range(NS - D2LAG, NS):
                r = d2(i)
                acc = r if acc is None else acc + r
            for q, s in enumerate(outs):
                for ct in range(C // 128):
                    fcur[s, ct] += acc[q * M:(q + 1) * M, ct * 128:(ct + 1) * 128]

    def sets(t):
        act = tuple(s for s in range(4) if 0 <= t - LAG * s < NB)
        pre = tuple(s for s in range(3) if 0 <= t - 1 - LAG * s < NB)
        return act, pre

    def when(cond, fn, arg):
        if isinstance(cond, bool):
            if cond:
                fn(arg)
        else:
            pl.when(cond)(lambda: fn(arg))

    def step(t, par, act, pre):
        when(t < NB, arrive, t)
        if isinstance(t, int) and t == 1:
            stage_x(4)

        def piece(n, _):
            def at(k, fn, arg):
                if isinstance(arg, int):
                    if arg < NB:
                        pl.when(n == k)(lambda: fn(arg))
                else:
                    pl.when(jnp.logical_and(n == k, arg < NB))(lambda: fn(arg))
            at(1, stage_r, t + 2)
            at(2, stage_d, t + 1)
            if not (isinstance(t, int) and t == 0):
                at(2, stage_x, t + 4)
            body(t, par, n, act, pre)
            return 0
        lax.fori_loop(0, NCH, piece, 0)

    part_r(0, 0)
    part_x(1, 1)
    part_r(0, 1)
    part_d(0, 0)
    part_r(1, 0)
    stage_x(2)
    part_d(0, 1)
    part_r(1, 1)
    stage_y(1)
    stage_x(3)
    nsteps = NB + 3 * LAG
    t = 0
    while t < nsteps:
        e = t
        while e < nsteps and sets(e) == sets(t):
            e += 1
        act, pre = sets(t)
        if e - t >= 4:
            def pair(u, _, t=t, act=act, pre=pre):
                for q in range(2):
                    step(t + 2 * u + q, (t + q) % 2, act, pre)
                return 0
            lax.fori_loop(0, (e - t) // 2, pair, 0)
        else:
            for tt in range(t, e):
                if tt in (1, 3):
                    stage_y(2 + tt // 2)
                step(tt, tt % 2, act, pre)
        t = e

    st = jnp.concatenate([jnp.sum(s_acc[k], axis=0, keepdims=True) for k in range(2)], 0)
    h1 = st.astype(bf16).astype(f32)
    h2 = (st - h1).astype(bf16).astype(f32)
    h3 = st - h1 - h2
    lhs = jnp.concatenate([h1, h2, h3, jnp.zeros((10, D), f32)], 0).astype(bf16)
    o = jnp.dot(lhs, wout_ref[...], preferred_element_type=f32)
    yv = x2 + (o[0:2] + (o[2:4] + o[4:6]))
    YP = (yp0, yp1, yp2)
    W = C // 3
    coords = (z, y, x)
    peers = (zpeers, ypeers, [xpeers[2], xpeers[0], xpeers[1]])
    views = (lambda r: r.at[0, 0, pl.ds(0, 3), 0], lambda r: r.at[0, pl.ds(0, 3), :, 0], lambda r: r.at[pl.ds(0, 3), :, :, 0], lambda r: r.at[:, :, :, 0])
    for p in range(3):
        YP[p][z, y, x, c] = yv[:, p * W:(p + 1) * W]

    def ywait(p, k):
        v = views[k](YP[p])
        pltpu.make_async_copy(v, v, y_sem.at[p, k]).wait()

    for k in range(4):
        for p in range(3):
            if k:
                ywait(p, k - 1)
            done = [(p + e) % 3 for e in range(k)]
            ref = YP[p].at[tuple(slice(None) if a in done else coords[a] for a in range(3)) + (c,)]
            for dev in (peers[(p + k) % 3] if k < 3 else [partner]):
                send(ref, ref, ysend_sem.at[p], y_sem.at[p, k], dev)
    for p in range(3):
        ywait(p, 3)
        for zz in range(4):
            for yy in range(4):
                for xx in (0, 2):
                    rows = [YP[p][zz, yy, xx + i // 2, i % 2] for i in range(4)]
                    y_ref[pl.ds((zz * 4 + yy) * 16 + xx * 4, 8), p * W:(p + 1) * W] = jnp.concatenate(rows, 0)

    def drain(ref, sem):
        for view in (ref.at[pl.ds(0, 63), 0], ref.at[:, 0]):
            pltpu.make_async_copy(view, view, sem).wait()
    drain(gb, send_sem)
    drain(hb, sendh_sem)
    for p in range(3):
        for view in views:
            v = view(YP[p])
            pltpu.make_async_copy(v, v, ysend_sem.at[p]).wait()


def solution(mesh):
    V = pltpu.VMEM
    dma = pltpu.SemaphoreType.DMA
    run = pl.pallas_call(
        kernel,
        out_shape=jax.ShapeDtypeStruct((256, C), f32),
        in_specs=[pl.BlockSpec(memory_space=pl.ANY)] * 5 + [pl.BlockSpec(memory_space=pltpu.SMEM)],
        out_specs=pl.BlockSpec(memory_space=pltpu.VMEM),
        scratch_shapes=[
            V((64, 2, 2, 8, D), bf16), V((64, 2, 8, 128), f32), V((C, D), bf16), V((D, C), bf16), V((8, C), f32),
            V((RING, J, D), f32), V((RING, J, D), f32),
            V((3 * M, C), bf16), V((3 * M, C), bf16), V((3, C // 128, M, 128), f32), V((3, C // 128, M, 128), f32),
            V((8, D), f32), V((3, 2, 8, C), f32), V((2, 8, D), f32), *[V((4, 4, 4, 2, 2, C // 3), f32) for _ in range(3)],
            dma((6,)), dma, dma, *[dma(n) for _ in range(4) for n in ((2, NB), (NB,))], dma((3,)), dma((3, 4)),
        ],
        compiler_params=pltpu.CompilerParams(vmem_limit_bytes=60 * 2**20, collective_id=0, has_side_effects=True),
    )

    def local_run(x_init, w_in, w_out, mod_gamma, mod_beta, step_size):
        y = run(x_init.reshape(256, C), w_in, w_out, mod_gamma, mod_beta, step_size)
        return y.reshape(x_init.shape)

    return jax.shard_map(local_run, mesh=mesh, in_specs=(P("data", None, None), P(None, None), P(None, None), P("time", None), P("time", None), P("time")), out_specs=P("data", None, None), check_vma=False)
```
